256 devices in a mesh: px: 32 (over z, x_lo, core), pz: 8 (over y, x_hi).
Axes of the slice: x: 4 (x_hi: 2, x_lo: 2; x = x_hi * 2 + x_lo), y: 4, z: 8, core: 2. Of those that a mesh axis runs over, the one named last changes fastest.
Arguments:
- base: float32 [3, 256, 256, 128], P(None, 'px', 'pz'), may hold values from -6 to 6
- adjoint: float32 [3, 256, 256, 128], P(None, 'px', 'pz'), may hold values from -6 to 6
- tangent: float32 [1, 3, 256, 256, 128], P(None, None, 'px', 'pz'), may hold values from -6 to 6
- second: float32 [1, 3, 256, 256, 128], P(None, None, 'px', 'pz'), may hold values from -6 to 6
- dealias_mask: int32 [256, 256], P('px', 'pz'), may hold values 0 or 1
- tau_rows: int32 [256, 256, 2], P('px', 'pz'), may hold values from 0 to 63
- tau_inverse: float32 [256, 256, 64, 128], P('px', 'pz'), may hold values from -1 to 2.5, as said below
Outputs:
- base_next: float32 [3, 256, 256, 128], P(None, 'px', 'pz')
- adjoint_next: float32 [3, 256, 256, 128], P(None, 'px', 'pz')
- tangent_next: float32 [1, 3, 256, 256, 128], P(None, None, 'px', 'pz')
- second_next: float32 [1, 3, 256, 256, 128], P(None, None, 'px', 'pz')
The draws below stay inside these ranges and needn't reach their ends.
Inputs may be any that keep to these rules, and one draw needn't show every extreme that they name: `tau_inverse`: entry [kx, kz, a, p * 64 + b] maps the input at Chebyshev index 2 b + p to the output at index 2 a + p.
All inputs are finite; a program needn't handle non-finite values. No bound on the sum of `dealias_mask` on one device may be relied on, other than what follows from the above.
Results may differ from the reference program's by a relative error of at most 0.00013.
Values sent between devices are 32-bit elements; how exact they have to be, the bound alone decides.
No kernel may reach another device: no remote copies, remote signals or barrier semaphores. Data moves between devices by JAX's collectives and lax.ppermute only.
A program may use at most 128 MiB of HBM per device.

```python
import math
import jax
import jax.numpy as jnp
from jax import lax

NX = 256
NZ = 256
NY = 128
DIRS = 1
HALF = 64


def draw_tau_inverse(key, part):
    shape = (NX, NZ, HALF, NY)
    key_noise = jax.random.fold_in(key, 11)
    key_diag = jax.random.fold_in(key, 23)
    spread = 0.6 / math.sqrt(HALF)
    noise = jnp.clip(jax.random.normal(key_noise, shape, jnp.float32), -4.0, 4.0) * spread
    diagonal = jax.random.uniform(key_diag, (NX, NZ, HALF, 2), jnp.float32, 0.5, 1.5)
    diagonal_full = jnp.repeat(diagonal, HALF, axis=3)
    outputs = jnp.arange(HALF, dtype=jnp.int32)[:, None]
    columns = jnp.arange(NY, dtype=jnp.int32)[None, :] % HALF
    identity = (outputs == columns)[None, None]
    return noise + jnp.where(identity, diagonal_full, jnp.zeros_like(diagonal_full))


def place_ends(array, key, least, top_value):
    spot = [jax.random.randint(jax.random.fold_in(key, axis), (), 0, length) for axis, length in enumerate(array.shape)]
    longest = array.shape.index(max(array.shape))
    beside = spot[:longest] + [(spot[longest] + 1) % array.shape[longest]] + spot[longest + 1:]
    return array.at[tuple(spot)].set(least).at[tuple(beside)].set(top_value)


def shard_levels(key, dims, cuts, smallest, top_value):
    factor_of, own = 1.0, jax.random.fold_in(key, 6)
    for position, shards_of in cuts:
        heights = jnp.exp(jax.random.uniform(jax.random.fold_in(own, position), (shards_of,), jnp.float32, smallest / len(cuts), top_value / len(cuts)))
        factor_of = factor_of * jnp.repeat(heights, dims[position] // shards_of).reshape([-1 if axis == position else 1 for axis in range(len(dims))])
    return factor_of


def gaussian(key, shape, scale, bound, split=(), held_as=jnp.bfloat16):
    values = scale * jax.random.normal(key, shape, jnp.float32)
    if split:
        values = values * shard_levels(key, shape, split, -0.22, 0.18)
    return jnp.clip(values, -bound, bound).astype(held_as)


def setup_inputs(seed: int = 0) -> dict:
    splits = jax.random.split(jax.random.key(seed), 8)
    base = gaussian(splits[0], (3, NX, NZ, NY), 1.0, 6.0, ((1, 32), (2, 8)), jnp.float32)
    adjoint = gaussian(splits[1], (3, NX, NZ, NY), 1.0, 6.0, ((1, 32), (2, 8)), jnp.float32)
    tangent = gaussian(splits[2], (DIRS, 3, NX, NZ, NY), 1.0, 6.0, ((2, 32), (3, 8)), jnp.float32)
    second = gaussian(splits[3], (DIRS, 3, NX, NZ, NY), 1.0, 6.0, ((2, 32), (3, 8)), jnp.float32)
    dealias_mask = place_ends((jax.random.randint(splits[4], (NX, NZ), 0, 3) < 2).astype(jnp.int32), jax.random.fold_in(splits[4], 1), 0, 1)
    tau_rows = place_ends(jax.random.randint(splits[5], (NX, NZ, 2), 0, HALF), jax.random.fold_in(splits[5], 1), 0, HALF - 1).astype(jnp.int32)
    tau_inverse = draw_tau_inverse(jax.random.fold_in(splits[7], 71), 0)
    return dict(base=base, adjoint=adjoint, tangent=tangent, second=second, dealias_mask=dealias_mask, tau_rows=tau_rows, tau_inverse=tau_inverse)


step_gain = 0.5

def hartley(length):
    indices = jnp.arange(length, dtype=jnp.int32)
    product = indices[:, None] * indices[None, :] % length
    angles = product.astype(jnp.float32) * (2.0 * math.pi / length)
    return (jnp.cos(angles) + jnp.sin(angles)) / math.sqrt(length)

def hartley_slope(length):
    indices = jnp.arange(length, dtype=jnp.int32)
    product = indices[:, None] * indices[None, :] % length
    angles = product.astype(jnp.float32) * (2.0 * math.pi / length)
    signed = jnp.where(indices < length // 2, indices, indices - length).astype(jnp.float32)
    return (jnp.cos(angles) - jnp.sin(angles)) * (signed * (2.0 * math.pi / length))[None, :] / math.sqrt(length)

def chebyshev(length):
    indices = jnp.arange(length, dtype=jnp.int32)
    product = (2 * indices[:, None] + 1) * indices[None, :] % (4 * length)
    angles = product.astype(jnp.float32) * (math.pi / (2 * length))
    column_scale = jnp.where(indices == 0, math.sqrt(1.0 / length), math.sqrt(2.0 / length)).astype(jnp.float32)
    return jnp.cos(angles) * column_scale[None, :]

def chebyshev_slope(length):
    indices = jnp.arange(length, dtype=jnp.int32)
    product = (2 * indices[:, None] + 1) * indices[None, :] % (4 * length)
    angles = product.astype(jnp.float32) * (math.pi / (2 * length))
    nodes = jnp.sin((2 * indices + 1).astype(jnp.float32) * (math.pi / (2 * length)))
    column_scale = jnp.where(indices == 0, math.sqrt(1.0 / length), math.sqrt(2.0 / length)).astype(jnp.float32)
    column_scale = column_scale * indices.astype(jnp.float32)
    return jnp.sin(angles) * column_scale[None, :] / (length * nodes[:, None])

def crossed(first, other, axis):
    return jnp.roll(first, -1, axis) * jnp.roll(other, -2, axis) - jnp.roll(first, -2, axis) * jnp.roll(other, -1, axis)

def forcings(velocity, vortex):
    grid_shape = velocity.shape[2:]
    base_v, adj_v = (velocity[0], velocity[1])
    tang_v, sec_v = (velocity[2:2 + DIRS], velocity[2 + DIRS:])
    base_o, adj_o = (vortex[0], vortex[1])
    tang_o, sec_o = (vortex[2:2 + DIRS], vortex[2 + DIRS:])
    force_base = crossed(base_v, base_o, 0)
    force_adjoint = crossed(base_v, adj_o, 0) + crossed(adj_v, base_o, 0)
    force_tangent = crossed(base_v[None], tang_o, 1) + crossed(tang_v, base_o[None], 1)
    force_second = crossed(base_v[None], sec_o, 1) + crossed(sec_v, base_o[None], 1) + crossed(tang_v, adj_o[None], 1) + crossed(adj_v[None], tang_o, 1)
    return jnp.concatenate([force_base, force_adjoint, force_tangent.reshape((3 * DIRS,) + grid_shape), force_second.reshape((3 * DIRS,) + grid_shape)], 0)

def to_physical(stacked, table_x, table_z, table_y):
    highest = lax.Precision.HIGHEST
    result = jnp.einsum('cxzn,jn->cxzj', stacked, table_y, precision=highest)
    result = jnp.einsum('cxkj,zk->cxzj', result, table_z, precision=highest)
    return jnp.einsum('ckzj,xk->cxzj', result, table_x, precision=highest)

def reference(base, adjoint, tangent, second, dealias_mask, tau_rows, tau_inverse):
    highest = lax.Precision.HIGHEST
    grid_shape = (NX, NZ, NY)
    count = 2 + 2 * DIRS
    hart_x = hartley(NX)
    hart_z = hartley(NZ)
    cheb_y = chebyshev(NY)
    stacked = jnp.concatenate([base, adjoint, tangent.reshape((3 * DIRS,) + grid_shape), second.reshape((3 * DIRS,) + grid_shape)], 0)
    fields = stacked.shape[0]
    values = to_physical(stacked, hart_x, hart_z, cheb_y).reshape((count, 3) + grid_shape)
    slope_x = to_physical(stacked, hartley_slope(NX), hart_z, cheb_y).reshape((count, 3) + grid_shape)
    slope_z = to_physical(stacked, hart_x, hartley_slope(NZ), cheb_y).reshape((count, 3) + grid_shape)
    slope_y = to_physical(stacked, hart_x, hart_z, chebyshev_slope(NY)).reshape((count, 3) + grid_shape)
    vortex = jnp.stack([slope_y[:, 2] - slope_z[:, 1], slope_z[:, 0] - slope_x[:, 2], slope_x[:, 1] - slope_y[:, 0]], 1)
    forcing = forcings(values, vortex)
    spectral = jnp.einsum('cxzj,xk->ckzj', forcing, hart_x, precision=highest)
    spectral = jnp.einsum('cxzj,zk->cxkj', spectral, hart_z, precision=highest)
    forcing_hat = jnp.einsum('cxzj,jn->cxzn', spectral, cheb_y, precision=highest)
    right_side = stacked + step_gain * forcing_hat * dealias_mask.astype(jnp.float32)[None, :, :, None]
    right_side = right_side.reshape((fields, NX, NZ, HALF, 2))
    kept_rows = jnp.arange(HALF, dtype=jnp.int32)[None, None, :, None] != tau_rows[:, :, None, :]
    right_side = jnp.where(kept_rows[None], right_side, jnp.zeros_like(right_side))
    blocks = tau_inverse.reshape((NX, NZ, HALF, 2, HALF))

    def solve_line(pieces):
        return jnp.einsum('zapb,czbp->czap', pieces[0], pieces[1], precision=highest)
    solved = lax.map(solve_line, (blocks, jnp.moveaxis(right_side, 1, 0)))
    solved = jnp.moveaxis(solved, 0, 1).reshape((fields,) + grid_shape)
    base_next = solved[0:3]
    adjoint_next = solved[3:6]
    tangent_next = solved[6:6 + 3 * DIRS].reshape((DIRS, 3) + grid_shape)
    second_next = solved[6 + 3 * DIRS:].reshape((DIRS, 3) + grid_shape)
    return (base_next, adjoint_next, tangent_next, second_next)
```

```python
import math

import jax
import jax.numpy as jnp
import numpy as np
from jax import lax
from jax.experimental import pallas as pl
from jax.experimental.pallas import tpu as pltpu
from jax.sharding import PartitionSpec as P

NX = 256
NZ = 256
NY = 128
HALF = 64
GX = 32
GZ = 8
LX = NX // GX
LZ = NZ // GZ
QY = NY // GX
BX = NX // GZ
F32 = jnp.float32
BF16 = jnp.bfloat16

step_gain = 0.5


def split_table(table):
    table = np.asarray(table, np.float32)
    high = table.astype(jnp.bfloat16)
    low = (table - high.astype(np.float32)).astype(jnp.bfloat16)
    return high, low


def hartley(length):
    index = np.arange(length)
    angle = (index[:, None] * index[None, :] % length) * (2.0 * math.pi / length)
    return (np.cos(angle) + np.sin(angle)) / math.sqrt(length)


def hartley_slope(length):
    index = np.arange(length)
    angle = (index[:, None] * index[None, :] % length) * (2.0 * math.pi / length)
    signed = np.where(index < length // 2, index, index - length)
    return (np.cos(angle) - np.sin(angle)) * (signed * (2.0 * math.pi / length))[None, :] / math.sqrt(length)


def chebyshev(length):
    index = np.arange(length)
    angle = ((2 * index[:, None] + 1) * index[None, :] % (4 * length)) * (math.pi / (2 * length))
    scale = np.where(index == 0, math.sqrt(1.0 / length), math.sqrt(2.0 / length))
    return np.cos(angle) * scale[None, :]


def chebyshev_slope(length):
    index = np.arange(length)
    angle = ((2 * index[:, None] + 1) * index[None, :] % (4 * length)) * (math.pi / (2 * length))
    nodes = np.sin((2 * index + 1) * (math.pi / (2 * length)))
    scale = np.where(index == 0, math.sqrt(1.0 / length), math.sqrt(2.0 / length)) * index
    return np.sin(angle) * scale[None, :] / (length * nodes[:, None])


def node_order():
    return (np.arange(GX)[None, :] * QY + np.arange(QY)[:, None]).reshape(-1)


def parity_order():
    return (2 * np.arange(HALF)[None, :] + np.arange(2)[:, None]).reshape(-1)


def tables():
    nodes = node_order()
    cheb = chebyshev(NY)
    both = np.concatenate([cheb[nodes], chebyshev_slope(NY)[nodes]], 0)
    both_hi, both_lo = split_table(both)
    y_first = np.concatenate([both_hi, both_hi], 1)
    y_second = both_lo
    hx_hi, hx_lo = split_table(hartley(NX))
    dx_hi, dx_lo = split_table(hartley_slope(NX))
    x_value = np.concatenate([hx_hi, hx_hi, hx_lo], 1)
    x_slope = np.concatenate([dx_hi, dx_hi, dx_lo], 1)
    hz_hi, hz_lo = split_table(hartley(NZ).T)
    dz_hi, dz_lo = split_table(hartley_slope(NZ).T)
    z_value = np.concatenate([hz_hi, hz_hi, hz_lo], 0)
    z_slope = np.concatenate([dz_hi, dz_hi, dz_lo], 0)
    order = parity_order()
    back_hi, back_lo = split_table(cheb[nodes][:, order])
    gather = (np.arange(NY)[:, None] == order[None, :]).astype(jnp.bfloat16)
    y_back = np.concatenate([back_hi, back_hi, back_lo, gather, gather], 0)
    place = gather.T
    even, odd = place[:HALF], place[HALF:]
    spread = np.concatenate([even, even, odd, odd] * 2, 0)
    return dict(y_first=y_first, y_second=y_second, x_value=x_value, x_slope=x_slope, z_value=z_value,
                z_slope=z_slope, y_back=y_back, spread=spread)


def dot(left, right):
    return lax.dot_general(left, right, (((1,), (0,)), ((), ())), preferred_element_type=F32)


def dot_nt(left, right):
    return lax.dot_general(left, right, (((1,), (1,)), ((), ())), preferred_element_type=F32)


def halves(array):
    high = array.astype(BF16)
    return high, (array - high.astype(F32)).astype(BF16)


def swap_strips(tiles):
    lane = lax.broadcasted_iota(jnp.int32, tiles[0].shape, 1)
    low = lane < 64
    even = (lane & 32) == 0
    first, second, third, fourth = tiles
    a = jnp.where(low, first, pltpu.roll(third, 64, 1))
    c = jnp.where(low, pltpu.roll(first, 64, 1), third)
    b = jnp.where(low, second, pltpu.roll(fourth, 64, 1))
    d = jnp.where(low, pltpu.roll(second, 64, 1), fourth)
    return [
        jnp.where(even, a, pltpu.roll(b, 32, 1)),
        jnp.where(even, pltpu.roll(a, 96, 1), b),
        jnp.where(even, c, pltpu.roll(d, 32, 1)),
        jnp.where(even, pltpu.roll(c, 96, 1), d),
    ]


def y_forward(velocities, first, second):
    count = len(velocities)
    stride = 5 * count * LX

    def kernel(*refs):
        sources, first_ref, second_ref, out_ref = refs[:count], refs[count], refs[count + 1], refs[count + 2]
        for v in range(count):
            for comp in range(3):
                rows = NY if comp == 1 else 2 * NY
                high, low = halves(sources[v][comp].reshape(LX * LZ, NY))
                result = dot_nt(first_ref[0:rows], jnp.concatenate([high, low], 1)) + dot_nt(second_ref[0:rows], high)
                for part in range(rows // NY):
                    field = 5 * v + (comp if part == 0 else 3 + comp // 2)
                    for quad in range(2):
                        tiles = [
                            result[part * NY + q * GX : part * NY + (q + 1) * GX, quad * 128 : (quad + 1) * 128]
                            for q in range(QY)
                        ]
                        for s, tile in enumerate(swap_strips(tiles)):
                            out_ref[pl.ds(field * LX + quad * 4 + s, GX, stride=stride), :] = tile

    out = pl.pallas_call(
        kernel,
        name="y_forward",
        out_shape=jax.ShapeDtypeStruct((GX * stride, 128), F32),
    )(*velocities, first, second)
    return out.reshape(GX, 5 * count, LX, 128)


def x_forward(received, value, slope):
    count = received.shape[1] // 5

    def kernel(in_ref, value_ref, slope_ref, out_ref):
        def one(v, carry):
            parts = [halves(in_ref[:, 5 * v + i].reshape(NX, 128)) for i in range(5)]
            high = jnp.concatenate([p[0] for p in parts], 1)
            low = jnp.concatenate([p[1] for p in parts], 1)
            stack = jnp.concatenate([high, low, high], 0)
            plain = dot(value_ref[...], stack)
            slopes = dot(slope_ref[...], stack[:, 128:384])
            u, vv, w, dyu, dyw = [plain[:, 128 * i : 128 * (i + 1)] for i in range(5)]
            dxv, dxw = slopes[:, :128], slopes[:, 128:]
            for i, piece in enumerate([u, vv, w, dyw, dxw, dxv - dyu]):
                out_ref[:, 6 * v + i] = piece.reshape(GZ, BX, 128)
            return carry

        lax.fori_loop(0, count, one, 0)

    return pl.pallas_call(
        kernel,
        name="x_forward",
        out_shape=jax.ShapeDtypeStruct((GZ, 6 * count, BX, 128), F32),
    )(received, value, slope)


def z_stage(received, value, slope):
    count = received.shape[1] // 6
    rows = QY * BX

    def kernel(in_ref, value_ref, slope_ref, out_ref, phys, force):
        def forward(v, carry):
            lefts = []
            for i in range(6):
                field = 6 * v + i
                sides = [swap_strips([in_ref[4 * side + h, field] for h in range(4)]) for side in range(2)]
                lines = jnp.concatenate(
                    [jnp.concatenate([sides[0][q], sides[1][q]], 1) for q in range(QY)], 0
                )
                high, low = halves(lines)
                lefts.append(jnp.concatenate([high, low, high], 1))
            values = dot(jnp.concatenate(lefts, 0), value_ref[...])
            slopes = dot(jnp.concatenate(lefts[0:2], 0), slope_ref[...])
            pieces = [values[rows * i : rows * (i + 1)] for i in range(6)]
            pieces[3] = pieces[3] - slopes[rows:]
            pieces[4] = slopes[:rows] - pieces[4]
            for i in range(6):
                phys[6 * v + i] = pieces[i]
            return carry

        lax.fori_loop(0, count, forward, 0)

        def cross_terms(r, carry):
            at = pl.ds(pl.multiple_of(r * 8, 8), 8)
            field = [phys[i, at, :] for i in range(24)]

            def cross(a, b):
                va, ob = field[6 * a : 6 * a + 3], field[6 * b + 3 : 6 * b + 6]
                return [va[(i + 1) % 3] * ob[(i + 2) % 3] - va[(i + 2) % 3] * ob[(i + 1) % 3] for i in range(3)]

            def total(*pairs):
                terms = [cross(a, b) for a, b in pairs]
                return [sum(t[i] for t in terms[1:]) + terms[0][i] if len(terms) > 1 else terms[0][i] for i in range(3)]

            results = (
                total((0, 0)) + total((0, 1), (1, 0)) + total((0, 2), (2, 0)) + total((0, 3), (3, 0), (2, 1), (1, 2))
            )
            for i, piece in enumerate(results):
                force[i, at, :] = piece
            return carry

        lax.fori_loop(0, rows // 8, cross_terms, 0)

        def backward(v, carry):
            lefts = []
            for i in range(3):
                high, low = halves(force[3 * v + i])
                lefts.append(jnp.concatenate([high, low, high], 1))
            result = dot(jnp.concatenate(lefts, 0), value_ref[...])
            for i in range(3):
                for side in range(2):
                    tiles = [
                        result[rows * i + q * BX : rows * i + (q + 1) * BX, 128 * side : 128 * (side + 1)]
                        for q in range(QY)
                    ]
                    for h, tile in enumerate(swap_strips(tiles)):
                        out_ref[4 * side + h, 3 * v + i] = tile
            return carry

        lax.fori_loop(0, count, backward, 0)

    return pl.pallas_call(
        kernel,
        name="z_stage",
        out_shape=jax.ShapeDtypeStruct((GZ, 3 * count, BX, 128), F32),
        scratch_shapes=[pltpu.VMEM((6 * count, rows, NZ), F32), pltpu.VMEM((3 * count, rows, NZ), F32)],
    )(received, value, slope)


def x_backward(received, value):
    fields = received.shape[1]

    def kernel(in_ref, value_ref, out_ref):
        def two(k, carry):
            parts = [halves(in_ref[:, 2 * k + i].reshape(NX, 128)) for i in range(2)]
            high = jnp.concatenate([p[0] for p in parts], 1)
            low = jnp.concatenate([p[1] for p in parts], 1)
            result = dot(value_ref[...], jnp.concatenate([high, low, high], 0))
            for i in range(2):
                out_ref[:, 2 * k + i] = result[:, 128 * i : 128 * (i + 1)].reshape(GX, LX, 128)
            return carry

        lax.fori_loop(0, fields // 2, two, 0)

    return pl.pallas_call(
        kernel,
        name="x_backward",
        out_shape=jax.ShapeDtypeStruct((GX, fields, LX, 128), F32),
    )(received, value)


def y_solve(received, velocities, gain, keep, tau_inverse, y_back, spread):
    fields = received.shape[1]
    lines = LX * LZ
    pad = 16
    stride = fields * LX

    def kernel(in_ref, *refs):
        sources = refs[:4]
        gain_ref, keep_ref, tau_ref, back_ref, spread_ref = refs[4:9]
        outs = refs[9:13]
        right, solved, solved_odd = refs[13:]
        step = pl.program_id(0)

        @pl.when(step == 0)
        def _():
            for f in range(fields):
                quads = []
                for quad in range(2):
                    tiles = swap_strips(
                        [in_ref[pl.ds(f * LX + quad * 4 + s, GX, stride=stride), :] for s in range(4)]
                    )
                    quads.append(jnp.concatenate(tiles, 0).T)
                high, low = halves(jnp.concatenate(quads, 0) * gain_ref[...])
                own_high, own_low = halves(sources[f // 3][f % 3].reshape(lines, NY))
                result = dot(jnp.concatenate([high, low, high, own_high, own_low], 1), back_ref[...])
                right[pl.ds(f, lines, stride=pad), :] = jnp.where(keep_ref[...] > 0.5, result, 0.0)

        lane = lax.broadcasted_iota(jnp.int32, (pad, NY), 1)
        first_half = lane < HALF
        zero = jnp.zeros((4 * pad, NY), BF16)

        def pair(k, carry):
            weights = []
            lefts = []
            for i in range(2):
                mode = 2 * k + i
                high, low = halves(tau_ref[0, mode])
                weights.append(jnp.concatenate([high, low], 0))
                line = right[pl.ds(pl.multiple_of((step * LZ + mode) * pad, pad), pad), :]
                even = halves(jnp.where(first_half, line, 0.0))
                odd = halves(jnp.where(first_half, 0.0, line))
                lefts.append(jnp.concatenate([even[0], odd[0], even[1], odd[1]], 0))
            left = jnp.concatenate(
                [jnp.concatenate([lefts[0], zero], 1), jnp.concatenate([zero, lefts[1]], 1)], 0
            )
            result = dot_nt(left, jnp.concatenate(weights, 1))
            for i in range(2):
                piece = result[4 * pad * i : 4 * pad * (i + 1)]
                piece = piece[: 2 * pad] + piece[2 * pad :]
                at = pl.ds(pl.multiple_of((2 * k + i) * pad, pad), pad)
                solved[at, :] = piece[:pad]
                solved_odd[at, :] = piece[pad:]
            return carry

        lax.fori_loop(0, LZ // 2, pair, 0, unroll=4)

        for f in range(fields):
            high0, low0 = halves(solved[pl.ds(f, LZ, stride=pad), :])
            high1, low1 = halves(solved_odd[pl.ds(f, LZ, stride=pad), :])
            result = dot(jnp.concatenate([high0, high1, low0, low1], 1), spread_ref[...])
            outs[f // 3][f % 3, 0] = result

    whole = lambda *shape: pl.BlockSpec(shape, lambda i: (0,) * len(shape))
    return pl.pallas_call(
        kernel,
        name="y_solve",
        grid=(LX,),
        in_specs=[
            whole(GX * stride, 128),
            *[whole(3, LX, LZ, NY) for _ in range(4)],
            whole(lines, NY),
            whole(lines, NY),
            pl.BlockSpec((1, LZ, HALF, NY), lambda i: (i, 0, 0, 0)),
            whole(5 * NY, NY),
            whole(4 * NY, NY),
        ],
        out_specs=[pl.BlockSpec((3, 1, LZ, NY), lambda i: (0, i, 0, 0)) for _ in range(4)],
        out_shape=[jax.ShapeDtypeStruct((3, LX, LZ, NY), F32) for _ in range(4)],
        scratch_shapes=[pltpu.VMEM((lines * pad, NY), F32), pltpu.VMEM((LZ * pad, NY), F32), pltpu.VMEM((LZ * pad, NY), F32)],
        compiler_params=pltpu.CompilerParams(dimension_semantics=("arbitrary",)),
    )(received.reshape(GX * stride, 128), *velocities, gain, keep, tau_inverse, y_back, spread)


def exchange(array, axis):
    return lax.all_to_all(array, axis, split_axis=0, concat_axis=0, tiled=True)


def body(base, adjoint, tangent, second, dealias_mask, tau_rows, tau_inverse):
    table = tables()
    velocities = [base, adjoint, tangent.reshape(adjoint.shape), second.reshape(adjoint.shape)]
    gain = jnp.broadcast_to((step_gain * dealias_mask.astype(F32)).reshape(LX * LZ, 1), (LX * LZ, NY))
    positions = jnp.arange(HALF, dtype=jnp.int32)
    keep = (positions != tau_rows.reshape(LX * LZ, 2)[:, :, None]).astype(F32).reshape(LX * LZ, NY)

    spectral = y_forward(velocities, table["y_first"], table["y_second"])
    whole_x = exchange(spectral, "px")
    partial = x_forward(whole_x, table["x_value"], table["x_slope"])
    whole_z = exchange(partial, "pz")
    returned = z_stage(whole_z, table["z_value"], table["z_slope"])
    mixed = exchange(returned, "pz")
    spectral_x = x_backward(mixed, table["x_value"])
    whole_y = exchange(spectral_x, "px")
    outs = y_solve(whole_y, velocities, gain, keep, tau_inverse, table["y_back"], table["spread"])
    return (outs[0], outs[1], outs[2].reshape(tangent.shape), outs[3].reshape(second.shape))


def solution(mesh):
    in_specs = (
        P(None, "px", "pz", None),
        P(None, "px", "pz", None),
        P(None, None, "px", "pz", None),
        P(None, None, "px", "pz", None),
        P("px", "pz"),
        P("px", "pz", None),
        P("px", "pz", None, None),
    )
    out_specs = (
        P(None, "px", "pz", None),
        P(None, "px", "pz", None),
        P(None, None, "px", "pz", None),
        P(None, None, "px", "pz", None),
    )
    return jax.shard_map(body, mesh=mesh, in_specs=in_specs, out_specs=out_specs, check_vma=False)
```

```python
import math

import jax
import jax.numpy as jnp
import numpy as np
from jax import lax
from jax.experimental import pallas as pl
from jax.experimental.pallas import tpu as pltpu
from jax.sharding import PartitionSpec as P

NX = 256
NZ = 256
NY = 128
HALF = 64
GX = 32
GZ = 8
LX = NX // GX
LZ = NZ // GZ
QY = NY // GX
BX = NX // GZ
F32 = jnp.float32
BF16 = jnp.bfloat16

step_gain = 0.5


def split_table(table):
    table = np.asarray(table, np.float32)
    high = table.astype(jnp.bfloat16)
    low = (table - high.astype(np.float32)).astype(jnp.bfloat16)
    return high, low


def hartley(length):
    index = np.arange(length)
    angle = (index[:, None] * index[None, :] % length) * (2.0 * math.pi / length)
    return (np.cos(angle) + np.sin(angle)) / math.sqrt(length)


def hartley_slope(length):
    index = np.arange(length)
    angle = (index[:, None] * index[None, :] % length) * (2.0 * math.pi / length)
    signed = np.where(index < length // 2, index, index - length)
    return (np.cos(angle) - np.sin(angle)) * (signed * (2.0 * math.pi / length))[None, :] / math.sqrt(length)


def chebyshev(length):
    index = np.arange(length)
    angle = ((2 * index[:, None] + 1) * index[None, :] % (4 * length)) * (math.pi / (2 * length))
    scale = np.where(index == 0, math.sqrt(1.0 / length), math.sqrt(2.0 / length))
    return np.cos(angle) * scale[None, :]


def chebyshev_slope(length):
    index = np.arange(length)
    angle = ((2 * index[:, None] + 1) * index[None, :] % (4 * length)) * (math.pi / (2 * length))
    nodes = np.sin((2 * index + 1) * (math.pi / (2 * length)))
    scale = np.where(index == 0, math.sqrt(1.0 / length), math.sqrt(2.0 / length)) * index
    return np.sin(angle) * scale[None, :] / (length * nodes[:, None])


def node_order():
    return (np.arange(GX)[None, :] * QY + np.arange(QY)[:, None]).reshape(-1)


def parity_order():
    return (2 * np.arange(HALF)[None, :] + np.arange(2)[:, None]).reshape(-1)


def beside(table):
    return np.concatenate(split_table(table), 1)


def tables():
    nodes = node_order()
    cheb = chebyshev(NY)
    both = np.concatenate([cheb[nodes], chebyshev_slope(NY)[nodes]], 0)
    order = parity_order()
    gather = (np.arange(NY)[:, None] == order[None, :]).astype(jnp.bfloat16)
    place = gather.T
    even, odd = place[:HALF], place[HALF:]
    return dict(
        y_first=beside(both),
        value=beside(hartley(NX)),
        x_slope=beside(hartley_slope(NX)),
        z_slope=beside(hartley_slope(NZ).T),
        y_back=np.concatenate([*split_table(cheb[nodes][:, order]), gather], 0),
        spread=np.concatenate([even, even, odd, odd], 0),
    )


def three(table):
    half = table.shape[1] // 2
    return jnp.concatenate([table[:, :half], table[:, :half], table[:, half:]], 1)


def near(array):
    return pltpu.with_memory_space_constraint(array, pltpu.VMEM)


def dot(left, right):
    return lax.dot_general(left, right, (((1,), (0,)), ((), ())), preferred_element_type=F32)


def dot_nt(left, right):
    return lax.dot_general(left, right, (((1,), (1,)), ((), ())), preferred_element_type=F32)


def halves(array):
    high = array.astype(BF16)
    return high, (array - high.astype(F32)).astype(BF16)


def swap_strips(tiles):
    lane = lax.broadcasted_iota(jnp.int32, tiles[0].shape, 1)
    low = lane < 64
    even = (lane & 32) == 0
    first, second, third, fourth = tiles
    a = jnp.where(low, first, pltpu.roll(third, 64, 1))
    c = jnp.where(low, pltpu.roll(first, 64, 1), third)
    b = jnp.where(low, second, pltpu.roll(fourth, 64, 1))
    d = jnp.where(low, pltpu.roll(second, 64, 1), fourth)
    return [
        jnp.where(even, a, pltpu.roll(b, 32, 1)),
        jnp.where(even, pltpu.roll(a, 96, 1), b),
        jnp.where(even, c, pltpu.roll(d, 32, 1)),
        jnp.where(even, pltpu.roll(c, 96, 1), d),
    ]


def y_forward(velocities, first):
    count = len(velocities)
    stride = 5 * count * LX

    def kernel(*refs):
        sources, first_ref, out_ref = refs[:count], refs[count], refs[count + 1]
        for v in range(count):
            for comp in range(3):
                rows = NY if comp == 1 else 2 * NY
                high, low = halves(sources[v][comp].reshape(LX * LZ, NY))
                result = dot_nt(three(first_ref[0:rows]), jnp.concatenate([high, low, high], 1))
                for part in range(rows // NY):
                    field = 5 * v + (comp if part == 0 else 3 + comp // 2)
                    for quad in range(2):
                        tiles = [
                            result[part * NY + q * GX : part * NY + (q + 1) * GX, quad * 128 : (quad + 1) * 128]
                            for q in range(QY)
                        ]
                        for s, tile in enumerate(swap_strips(tiles)):
                            out_ref[pl.ds(field * LX + quad * 4 + s, GX, stride=stride), :] = tile

    out = pl.pallas_call(
        kernel,
        name="y_forward",
        out_shape=jax.ShapeDtypeStruct((GX * stride, 128), F32),
    )(*velocities, first)
    return out.reshape(GX, 5 * count, LX, 128)


def fill_blocks(target_ref, first_row, source_ref, first_lane, lanes, position):
    for k in range(GZ):
        start = pl.multiple_of((position ^ k) * BX, BX)
        row = first_row + k * BX
        target_ref[row : row + BX, :] = source_ref[pl.ds(start, BX), first_lane : first_lane + lanes]


def fill_rows(target_ref, source_ref, position):
    for group, lane in enumerate((0, 0, NZ)):
        fill_blocks(target_ref, group * NZ, source_ref, lane, NZ, position)


def x_forward(received, value, slope, position=None):
    count = received.shape[1] // 5
    parts_out = position is not None

    def kernel(*refs):
        if parts_out:
            position_ref, in_ref, value_ref, slope_ref = refs[:4]
            outs = refs[4 : 4 + GZ]
            value_own, slope_own = refs[4 + GZ :]
            fill_blocks(value_own, 0, value_ref, 0, 2 * NX, position_ref[0])
            fill_blocks(slope_own, 0, slope_ref, 0, 2 * NX, position_ref[0])
        else:
            in_ref, value_own, slope_own, out_ref = refs

        @pl.loop(0, count)
        def _(v):
            parts = [halves(in_ref[:, 5 * v + i].reshape(NX, 128)) for i in range(5)]
            high = jnp.concatenate([p[0] for p in parts], 1)
            low = jnp.concatenate([p[1] for p in parts], 1)
            stack = jnp.concatenate([high, low, high], 0)
            plain = dot(three(value_own[...]), stack)
            slopes = dot(three(slope_own[...]), stack[:, 128:384])
            u, vv, w, dyu, dyw = [plain[:, 128 * i : 128 * (i + 1)] for i in range(5)]
            dxv, dxw = slopes[:, :128], slopes[:, 128:]
            for i, piece in enumerate([u, vv, w, dyw, dxw, dxv - dyu]):
                if parts_out:
                    for k in range(GZ):
                        outs[k][6 * v + i] = piece[k * BX : (k + 1) * BX]
                else:
                    out_ref[:, 6 * v + i] = piece.reshape(GZ, BX, 128)

    vmem = pl.BlockSpec(memory_space=pltpu.VMEM)
    if parts_out:
        return pl.pallas_call(
            kernel,
            name="x_forward_parts",
            in_specs=[pl.BlockSpec(memory_space=pltpu.SMEM), vmem, vmem, vmem],
            out_shape=[jax.ShapeDtypeStruct((6 * count, BX, 128), F32)] * GZ,
            scratch_shapes=[pltpu.VMEM((NX, 2 * NX), BF16), pltpu.VMEM((NX, 2 * NX), BF16)],
        )(position, near(received), value, slope)
    return pl.pallas_call(
        kernel,
        name="x_forward",
        in_specs=[vmem, vmem, vmem],
        out_shape=jax.ShapeDtypeStruct((GZ, 6 * count, BX, 128), F32),
    )(near(received), value, slope)


ROWS = QY * BX


def cross(velocity, vortex):
    return [
        velocity[(i + 1) % 3] * vortex[(i + 2) % 3] - velocity[(i + 2) % 3] * vortex[(i + 1) % 3] for i in range(3)
    ]


def added(*terms):
    result = terms[0]
    for term in terms[1:]:
        result = [a + b for a, b in zip(result, term)]
    return result


def z_stage(received, value, slope, position, earlier=None):
    split_in = isinstance(received, (list, tuple))
    inputs = list(received) if split_in else [received]
    count = 2
    keep = earlier is None

    def kernel(*refs):
        position_ref = refs[0]
        in_refs = refs[1 : 1 + len(inputs)]
        at = 1 + len(inputs)
        value_ref, slope_ref = refs[at : at + 2]
        at += 2
        if not keep:
            old = refs[at]
            at += 1
        outs = refs[at : at + GZ]
        at += GZ
        if keep:
            phys = refs[at]
            at += 1
        force, value_own, slope_own, back_own = refs[at : at + 4]
        if not keep:
            phys = refs[at + 4]
        fill_blocks(back_own, 0, value_ref, 0, 2 * NZ, position_ref[0])
        order = position_ref[0] if split_in else 0
        fill_rows(value_own, value_ref, order)
        fill_rows(slope_own, slope_ref, order)
        if split_in:
            source = lambda block, field: in_refs[block][field]
        else:
            source = lambda block, field: in_refs[0][block, field]

        @pl.loop(0, count)
        def _(v):
            lefts = []
            for i in range(6):
                sides = [swap_strips([source(4 * side + h, 6 * v + i) for h in range(4)]) for side in range(2)]
                lines = jnp.concatenate(
                    [jnp.concatenate([sides[0][q], sides[1][q]], 1) for q in range(QY)], 0
                )
                high, low = halves(lines)
                lefts.append(jnp.concatenate([high, low, high], 1))
            values = dot(jnp.concatenate(lefts, 0), value_own[...])
            slopes = dot(jnp.concatenate(lefts[0:2], 0), slope_own[...])
            pieces = [values[ROWS * i : ROWS * (i + 1)] for i in range(6)]
            pieces[3] = pieces[3] - slopes[ROWS:]
            pieces[4] = slopes[:ROWS] - pieces[4]
            for i in range(6):
                phys[6 * v + i] = pieces[i]

        def cross_terms(r, carry):
            rows = pl.ds(pl.multiple_of(r * 8, 8), 8)
            new = [phys[i, rows, :] for i in range(12)]
            if keep:
                base_v, base_o, adj_v, adj_o = new[0:3], new[3:6], new[6:9], new[9:12]
                results = cross(base_v, base_o) + added(cross(base_v, adj_o), cross(adj_v, base_o))
            else:
                past = [old[i, rows, :] for i in range(12)]
                base_v, base_o, adj_v, adj_o = past[0:3], past[3:6], past[6:9], past[9:12]
                tang_v, tang_o, sec_v, sec_o = new[0:3], new[3:6], new[6:9], new[9:12]
                results = added(cross(base_v, tang_o), cross(tang_v, base_o)) + added(
                    cross(base_v, sec_o), cross(sec_v, base_o), cross(tang_v, adj_o), cross(adj_v, tang_o)
                )
            for i, piece in enumerate(results):
                force[i, rows, :] = piece
            return carry

        lax.fori_loop(0, ROWS // 8, cross_terms, 0, unroll=2)

        @pl.loop(0, count)
        def _(v):
            lefts = []
            for i in range(3):
                high, low = halves(force[3 * v + i])
                lefts.append(jnp.concatenate([high, low, high], 1))
            result = dot_nt(jnp.concatenate(lefts, 0), three(back_own[...]))
            for i in range(3):
                for side in range(2):
                    tiles = [
                        result[ROWS * i + q * BX : ROWS * i + (q + 1) * BX, 128 * side : 128 * (side + 1)]
                        for q in range(QY)
                    ]
                    for h, tile in enumerate(swap_strips(tiles)):
                        outs[4 * side + h][3 * v + i] = tile

    vmem = pl.BlockSpec(memory_space=pltpu.VMEM)
    extra = [] if keep else [earlier]
    grid_fields = jax.ShapeDtypeStruct((6 * count, ROWS, NZ), F32)
    scratch = [
        pltpu.VMEM((3 * count, ROWS, NZ), F32),
        pltpu.VMEM((3 * NZ, NZ), BF16),
        pltpu.VMEM((3 * NZ, NZ), BF16),
        pltpu.VMEM((NZ, 2 * NZ), BF16),
    ]
    if not keep:
        scratch.append(pltpu.VMEM((6 * count, ROWS, NZ), F32))
    result = pl.pallas_call(
        kernel,
        name="z_stage_first" if keep else "z_stage_second",
        in_specs=[pl.BlockSpec(memory_space=pltpu.SMEM)] + [vmem] * (len(inputs) + 2 + len(extra)),
        out_shape=[jax.ShapeDtypeStruct((3 * count, BX, 128), F32)] * GZ + ([grid_fields] if keep else []),
        scratch_shapes=scratch,
    )(position, *[near(a) for a in inputs], value, slope, *extra)
    return result[:GZ], (result[GZ] if keep else None)


def x_backward(received, value, position):
    fields = received[0].shape[0]

    def kernel(*refs):
        position_ref = refs[0]
        in_refs = refs[1 : 1 + GZ]
        value_ref, out_ref, lines = refs[1 + GZ :]
        for k in range(GZ):
            start = pl.multiple_of((position_ref[0] ^ k) * BX, BX)
            lines[:, pl.ds(start, BX), :] = in_refs[k][...]
        for pair in range(fields // 2):
            parts = [halves(lines[2 * pair + i]) for i in range(2)]
            high = jnp.concatenate([p[0] for p in parts], 1)
            low = jnp.concatenate([p[1] for p in parts], 1)
            result = dot(three(value_ref[...]), jnp.concatenate([high, low, high], 0))
            for i in range(2):
                out_ref[:, 2 * pair + i] = result[:, 128 * i : 128 * (i + 1)].reshape(GX, LX, 128)

    vmem = pl.BlockSpec(memory_space=pltpu.VMEM)
    return pl.pallas_call(
        kernel,
        name="x_backward",
        in_specs=[pl.BlockSpec(memory_space=pltpu.SMEM)] + [vmem] * (GZ + 1),
        out_shape=jax.ShapeDtypeStruct((GX, fields, LX, 128), F32),
        scratch_shapes=[pltpu.VMEM((fields, NX, 128), F32)],
    )(position, *[near(a) for a in received], value)


PAD = 8


def y_backward(received, velocities, gain, keep, y_back):
    fields = received.shape[1]
    lines = LX * LZ
    stride = fields * LX

    def kernel(in_ref, first, second, gain_ref, keep_ref, back_ref, right):
        sources = [first, second]
        for v in range(2):
            lefts = []
            for comp in range(3):
                f = 3 * v + comp
                quads = []
                for quad in range(2):
                    tiles = swap_strips(
                        [in_ref[pl.ds(f * LX + quad * 4 + s, GX, stride=stride), :] for s in range(4)]
                    )
                    quads.append(jnp.concatenate(tiles, 0).T)
                high, low = halves(jnp.concatenate(quads, 0) * gain_ref[...])
                own_high, own_low = halves(sources[v][comp].reshape(lines, NY))
                lefts.append(jnp.concatenate([high, low, high, own_high, own_low], 1))
            high, low, own = back_ref[0:NY], back_ref[NY : 2 * NY], back_ref[2 * NY : 3 * NY]
            result = dot(jnp.concatenate(lefts, 0), jnp.concatenate([high, high, low, own, own], 0))
            for comp in range(3):
                line = result[lines * comp : lines * (comp + 1)]
                right[pl.ds(3 * v + comp, lines, stride=PAD), :] = jnp.where(keep_ref[...] > 0.5, line, 0.0)

        for f in range(fields, PAD):
            right[pl.ds(f, lines, stride=PAD), :] = jnp.zeros((lines, NY), F32)

    vmem = pl.BlockSpec(memory_space=pltpu.VMEM)
    return pl.pallas_call(
        kernel,
        name="y_backward",
        in_specs=[vmem] * 6,
        out_shape=jax.ShapeDtypeStruct((lines * PAD, NY), F32),
    )(near(received.reshape(GX * stride, 128)), *velocities, near(gain), near(keep), y_back)


def solve(first, second, tau_inverse, spread):
    pad = 2 * PAD

    def kernel(first_ref, second_ref, tau_ref, spread_ref, *refs):
        outs = refs[:4]
        solved, solved_odd = refs[4:]
        lane = lax.broadcasted_iota(jnp.int32, (pad, NY), 1)
        first_half = lane < HALF
        zero = jnp.zeros((4 * pad, NY), BF16)

        def pair(k, carry):
            weights = []
            lefts = []
            for i in range(2):
                mode = 2 * k + i
                high, low = halves(tau_ref[0, mode])
                weights.append(jnp.concatenate([high, low], 0))
                at = pl.ds(pl.multiple_of(mode * PAD, PAD), PAD)
                line = jnp.concatenate([first_ref[at, :], second_ref[at, :]], 0)
                even = halves(jnp.where(first_half, line, 0.0))
                odd = halves(jnp.where(first_half, 0.0, line))
                lefts.append(jnp.concatenate([even[0], odd[0], even[1], odd[1]], 0))
            left = jnp.concatenate(
                [jnp.concatenate([lefts[0], zero], 1), jnp.concatenate([zero, lefts[1]], 1)], 0
            )
            result = dot_nt(left, jnp.concatenate(weights, 1))
            for i in range(2):
                piece = result[4 * pad * i : 4 * pad * (i + 1)]
                piece = piece[: 2 * pad] + piece[2 * pad :]
                at = pl.ds(pl.multiple_of((2 * k + i) * pad, pad), pad)
                solved[at, :] = piece[:pad]
                solved_odd[at, :] = piece[pad:]
            return carry

        lax.fori_loop(0, LZ // 2, pair, 0, unroll=8)

        highs, lows = [], []
        for f in range(12):
            row = f if f < 6 else f + PAD - 6
            high0, low0 = halves(solved[pl.ds(row, LZ, stride=pad), :])
            high1, low1 = halves(solved_odd[pl.ds(row, LZ, stride=pad), :])
            highs.append(jnp.concatenate([high0, high1], 1))
            lows.append(jnp.concatenate([low0, low1], 1))
        result = dot(jnp.concatenate(highs + lows, 0), spread_ref[...])
        for f in range(12):
            outs[f // 3][f % 3, 0] = result[LZ * f : LZ * (f + 1)] + result[LZ * (12 + f) : LZ * (13 + f)]

    return pl.pallas_call(
        kernel,
        name="solve",
        grid=(LX,),
        in_specs=[
            pl.BlockSpec((LZ * PAD, NY), lambda i: (i, 0)),
            pl.BlockSpec((LZ * PAD, NY), lambda i: (i, 0)),
            pl.BlockSpec((1, LZ, HALF, NY), lambda i: (i, 0, 0, 0)),
            pl.BlockSpec((2 * NY, NY), lambda i: (0, 0)),
        ],
        out_specs=[pl.BlockSpec((3, 1, LZ, NY), lambda i: (0, i, 0, 0)) for _ in range(4)],
        out_shape=[jax.ShapeDtypeStruct((3, LX, LZ, NY), F32) for _ in range(4)],
        scratch_shapes=[pltpu.VMEM((LZ * pad, NY), F32), pltpu.VMEM((LZ * pad, NY), F32)],
        compiler_params=pltpu.CompilerParams(dimension_semantics=("arbitrary",)),
    )(first, second, tau_inverse, spread)


def exchange(array, axis):
    return lax.all_to_all(array, axis, split_axis=0, concat_axis=0, tiled=True)


def exchange_parts(parts):
    return [parts[0]] + [lax.ppermute(parts[k], "pz", [(i, i ^ k) for i in range(GZ)]) for k in range(1, GZ)]


def body(base, adjoint, tangent, second, dealias_mask, tau_rows, tau_inverse):
    table = tables()
    one = [base, adjoint]
    two = [tangent.reshape(adjoint.shape), second.reshape(adjoint.shape)]
    position = lax.axis_index("pz").astype(jnp.int32).reshape(1)
    gain = jnp.broadcast_to((step_gain * dealias_mask.astype(F32)).reshape(LX * LZ, 1), (LX * LZ, NY))
    rows = tau_rows.reshape(LX * LZ, 2)[:, :, None]
    keep = (jnp.arange(HALF, dtype=jnp.int32) != rows).astype(F32).reshape(LX * LZ, NY)
    sent_one = y_forward(one, table["y_first"])
    whole_one = exchange(sent_one, "px")
    sent_two = y_forward(two, table["y_first"])
    whole_two = exchange(sent_two, "px")
    parts_one = x_forward(whole_one, table["value"], table["x_slope"], position)
    lines_one = exchange_parts(parts_one)
    partial_two = x_forward(whole_two, table["value"], table["x_slope"])
    lines_two = exchange(partial_two, "pz")
    back_one, grid_one = z_stage(lines_one, table["value"], table["z_slope"], position)
    mixed_one = exchange_parts(back_one)
    modes_one = x_backward(mixed_one, table["value"], position)
    nodes_one = exchange(modes_one, "px")
    back_two, _ = z_stage(
        lines_two, table["value"], table["z_slope"], position, grid_one
    )
    mixed_two = exchange_parts(back_two)
    modes_two = x_backward(mixed_two, table["value"], position)
    nodes_two = exchange(modes_two, "px")
    right_one = y_backward(nodes_one, one, gain, keep, table["y_back"])
    right_two = y_backward(nodes_two, two, gain, keep, table["y_back"])
    outs = solve(right_one, right_two, tau_inverse, table["spread"])
    return (outs[0], outs[1], outs[2].reshape(tangent.shape), outs[3].reshape(second.shape))


def solution(mesh):
    in_specs = (
        P(None, "px", "pz", None),
        P(None, "px", "pz", None),
        P(None, None, "px", "pz", None),
        P(None, None, "px", "pz", None),
        P("px", "pz"),
        P("px", "pz", None),
        P("px", "pz", None, None),
    )
    out_specs = (
        P(None, "px", "pz", None),
        P(None, "px", "pz", None),
        P(None, None, "px", "pz", None),
        P(None, None, "px", "pz", None),
    )
    return jax.shard_map(body, mesh=mesh, in_specs=in_specs, out_specs=out_specs, check_vma=False)
```

```python
import math

import jax
import jax.numpy as jnp
import numpy as np
from jax import lax
from jax.experimental import pallas as pl
from jax.experimental.pallas import tpu as pltpu
from jax.sharding import PartitionSpec as P

NX = 256
NZ = 256
NY = 128
HALF = 64
GX = 32
GZ = 8
LX = NX // GX
LZ = NZ // GZ
QY = NY // GX
BX = NX // GZ
F32 = jnp.float32
BF16 = jnp.bfloat16

step_gain = 0.5


def split_table(table):
    table = np.asarray(table, np.float32)
    high = table.astype(jnp.bfloat16)
    low = (table - high.astype(np.float32)).astype(jnp.bfloat16)
    return high, low


def hartley(length):
    index = np.arange(length)
    angle = (index[:, None] * index[None, :] % length) * (2.0 * math.pi / length)
    return (np.cos(angle) + np.sin(angle)) / math.sqrt(length)


def hartley_slope(length):
    index = np.arange(length)
    angle = (index[:, None] * index[None, :] % length) * (2.0 * math.pi / length)
    signed = np.where(index < length // 2, index, index - length)
    return (np.cos(angle) - np.sin(angle)) * (signed * (2.0 * math.pi / length))[None, :] / math.sqrt(length)


def chebyshev(length):
    index = np.arange(length)
    angle = ((2 * index[:, None] + 1) * index[None, :] % (4 * length)) * (math.pi / (2 * length))
    scale = np.where(index == 0, math.sqrt(1.0 / length), math.sqrt(2.0 / length))
    return np.cos(angle) * scale[None, :]


def chebyshev_slope(length):
    index = np.arange(length)
    angle = ((2 * index[:, None] + 1) * index[None, :] % (4 * length)) * (math.pi / (2 * length))
    nodes = np.sin((2 * index + 1) * (math.pi / (2 * length)))
    scale = np.where(index == 0, math.sqrt(1.0 / length), math.sqrt(2.0 / length)) * index
    return np.sin(angle) * scale[None, :] / (length * nodes[:, None])


def node_order():
    return (np.arange(GX)[None, :] * QY + np.arange(QY)[:, None]).reshape(-1)


def parity_order():
    return (2 * np.arange(HALF)[None, :] + np.arange(2)[:, None]).reshape(-1)


def beside(table):
    return np.concatenate(split_table(table), 1)


def tables():
    nodes = node_order()
    cheb = chebyshev(NY)
    both = np.concatenate([cheb[nodes], chebyshev_slope(NY)[nodes]], 0)
    order = parity_order()
    gather = (np.arange(NY)[:, None] == order[None, :]).astype(jnp.bfloat16)
    place = gather.T
    even, odd = place[:HALF], place[HALF:]
    return dict(
        y_first=beside(both),
        value=beside(hartley(NX)),
        x_slope=beside(hartley_slope(NX)),
        z_slope=beside(hartley_slope(NZ).T),
        y_back=np.concatenate([*split_table(cheb[nodes][:, order]), gather], 0),
        spread=np.concatenate([even, even, odd, odd], 0),
    )


def three(table):
    half = table.shape[1] // 2
    return jnp.concatenate([table[:, :half], table[:, :half], table[:, half:]], 1)


def near(array):
    return pltpu.with_memory_space_constraint(array, pltpu.VMEM)


def dot(left, right):
    return lax.dot_general(left, right, (((1,), (0,)), ((), ())), preferred_element_type=F32)


def dot_nt(left, right):
    return lax.dot_general(left, right, (((1,), (1,)), ((), ())), preferred_element_type=F32)


def halves(array):
    high = array.astype(BF16)
    return high, (array - high.astype(F32)).astype(BF16)


def swap_strips(tiles):
    lane = lax.broadcasted_iota(jnp.int32, tiles[0].shape, 1)
    low = lane < 64
    even = (lane & 32) == 0
    first, second, third, fourth = tiles
    a = jnp.where(low, first, pltpu.roll(third, 64, 1))
    c = jnp.where(low, pltpu.roll(first, 64, 1), third)
    b = jnp.where(low, second, pltpu.roll(fourth, 64, 1))
    d = jnp.where(low, pltpu.roll(second, 64, 1), fourth)
    return [
        jnp.where(even, a, pltpu.roll(b, 32, 1)),
        jnp.where(even, pltpu.roll(a, 96, 1), b),
        jnp.where(even, c, pltpu.roll(d, 32, 1)),
        jnp.where(even, pltpu.roll(c, 96, 1), d),
    ]


def y_forward(velocities, first, compact):
    count = len(velocities)
    stride = 5 * count * LX

    def kernel(*refs):
        sources, first_ref, out_ref = refs[:count], refs[count], refs[count + 1]

        def one(source, rows, fields):
            high, low = halves(source.reshape(LX * LZ, NY))
            result = dot_nt(three(first_ref[0:rows]), jnp.concatenate([high, low, high], 1))
            for part, field in enumerate(fields):
                for quad in range(2):
                    tiles = [
                        result[part * NY + q * GX : part * NY + (q + 1) * GX, quad * 128 : (quad + 1) * 128]
                        for q in range(QY)
                    ]
                    for s, tile in enumerate(swap_strips(tiles)):
                        out_ref[pl.ds(field * LX + quad * 4 + s, GX, stride=stride), :] = tile

        for v in range(count):

            if compact:

                @pl.loop(0, 2)
                def _(i):
                    one(sources[v][2 * i], 2 * NY, (5 * v + 2 * i, 5 * v + 3 + i))

            else:
                for i in range(2):
                    one(sources[v][2 * i], 2 * NY, (5 * v + 2 * i, 5 * v + 3 + i))

            one(sources[v][1], NY, (5 * v + 1,))

    out = pl.pallas_call(
        kernel,
        name="y_forward",
        out_shape=jax.ShapeDtypeStruct((GX * stride, 128), F32),
    )(*velocities, first)
    return out.reshape(GX, 5 * count, LX, 128)


def fill_blocks(target_ref, first_row, source_ref, first_lane, lanes, position):
    for k in range(GZ):
        start = pl.multiple_of((position ^ k) * BX, BX)
        row = first_row + k * BX
        target_ref[row : row + BX, :] = source_ref[pl.ds(start, BX), first_lane : first_lane + lanes]


def fill_rows(target_ref, source_ref, position):
    for group, lane in enumerate((0, 0, NZ)):
        fill_blocks(target_ref, group * NZ, source_ref, lane, NZ, position)


def x_forward(received, value, slope, position=None):
    count = received.shape[1] // 5
    parts_out = position is not None

    def kernel(*refs):
        if parts_out:
            position_ref, in_ref, value_ref, slope_ref = refs[:4]
            outs = refs[4 : 4 + GZ]
            value_own, slope_own = refs[4 + GZ :]
            fill_blocks(value_own, 0, value_ref, 0, 2 * NX, position_ref[0])
            fill_blocks(slope_own, 0, slope_ref, 0, 2 * NX, position_ref[0])
        else:
            in_ref, value_own, slope_own, out_ref = refs

        @pl.loop(0, count)
        def _(v):
            parts = [halves(in_ref[:, 5 * v + i].reshape(NX, 128)) for i in range(5)]
            high = jnp.concatenate([p[0] for p in parts], 1)
            low = jnp.concatenate([p[1] for p in parts], 1)
            stack = jnp.concatenate([high, low, high], 0)
            plain = dot(three(value_own[...]), stack)
            slopes = dot(three(slope_own[...]), stack[:, 128:384])
            u, vv, w, dyu, dyw = [plain[:, 128 * i : 128 * (i + 1)] for i in range(5)]
            dxv, dxw = slopes[:, :128], slopes[:, 128:]
            for i, piece in enumerate([u, vv, w, dyw, dxw, dxv - dyu]):
                if parts_out:
                    for k in range(GZ):
                        outs[k][6 * v + i] = piece[k * BX : (k + 1) * BX]
                else:
                    out_ref[:, 6 * v + i] = piece.reshape(GZ, BX, 128)

    vmem = pl.BlockSpec(memory_space=pltpu.VMEM)
    if parts_out:
        return pl.pallas_call(
            kernel,
            name="x_forward_parts",
            in_specs=[pl.BlockSpec(memory_space=pltpu.SMEM), vmem, vmem, vmem],
            out_shape=[jax.ShapeDtypeStruct((6 * count, BX, 128), F32)] * GZ,
            scratch_shapes=[pltpu.VMEM((NX, 2 * NX), BF16), pltpu.VMEM((NX, 2 * NX), BF16)],
        )(position, near(received), value, slope)
    return pl.pallas_call(
        kernel,
        name="x_forward",
        in_specs=[vmem, vmem, vmem],
        out_shape=jax.ShapeDtypeStruct((GZ, 6 * count, BX, 128), F32),
    )(near(received), value, slope)


ROWS = QY * BX


def cross(velocity, vortex):
    return [
        velocity[(i + 1) % 3] * vortex[(i + 2) % 3] - velocity[(i + 2) % 3] * vortex[(i + 1) % 3] for i in range(3)
    ]


def added(*terms):
    result = terms[0]
    for term in terms[1:]:
        result = [a + b for a, b in zip(result, term)]
    return result


def z_stage(received, value, slope, position, earlier=None):
    split_in = isinstance(received, (list, tuple))
    inputs = list(received) if split_in else [received]
    count = 2
    keep = earlier is None

    def kernel(*refs):
        position_ref = refs[0]
        in_refs = refs[1 : 1 + len(inputs)]
        at = 1 + len(inputs)
        value_ref, slope_ref = refs[at : at + 2]
        at += 2
        if not keep:
            old = refs[at]
            at += 1
        outs = refs[at : at + GZ]
        at += GZ
        if keep:
            phys = refs[at]
            at += 1
        force, value_own, slope_own, back_own = refs[at : at + 4]
        if not keep:
            phys = refs[at + 4]
        fill_blocks(back_own, 0, value_ref, 0, 2 * NZ, position_ref[0])
        order = position_ref[0] if split_in else 0
        fill_rows(value_own, value_ref, order)
        fill_rows(slope_own, slope_ref, order)
        if split_in:
            source = lambda block, field: in_refs[block][field]
        else:
            source = lambda block, field: in_refs[0][block, field]

        @pl.loop(0, count)
        def _(v):
            lefts = []
            for i in range(6):
                sides = [swap_strips([source(4 * side + h, 6 * v + i) for h in range(4)]) for side in range(2)]
                lines = jnp.concatenate(
                    [jnp.concatenate([sides[0][q], sides[1][q]], 1) for q in range(QY)], 0
                )
                high, low = halves(lines)
                lefts.append(jnp.concatenate([high, low, high], 1))
            values = dot(jnp.concatenate(lefts, 0), value_own[...])
            slopes = dot(jnp.concatenate(lefts[0:2], 0), slope_own[...])
            pieces = [values[ROWS * i : ROWS * (i + 1)] for i in range(6)]
            pieces[3] = pieces[3] - slopes[ROWS:]
            pieces[4] = slopes[:ROWS] - pieces[4]
            for i in range(6):
                phys[6 * v + i] = pieces[i]

        def cross_terms(r, carry):
            rows = pl.ds(pl.multiple_of(r * 8, 8), 8)
            new = [phys[i, rows, :] for i in range(12)]
            if keep:
                base_v, base_o, adj_v, adj_o = new[0:3], new[3:6], new[6:9], new[9:12]
                results = cross(base_v, base_o) + added(cross(base_v, adj_o), cross(adj_v, base_o))
            else:
                past = [old[i, rows, :] for i in range(12)]
                base_v, base_o, adj_v, adj_o = past[0:3], past[3:6], past[6:9], past[9:12]
                tang_v, tang_o, sec_v, sec_o = new[0:3], new[3:6], new[6:9], new[9:12]
                results = added(cross(base_v, tang_o), cross(tang_v, base_o)) + added(
                    cross(base_v, sec_o), cross(sec_v, base_o), cross(tang_v, adj_o), cross(adj_v, tang_o)
                )
            for i, piece in enumerate(results):
                force[i, rows, :] = piece
            return carry

        lax.fori_loop(0, ROWS // 8, cross_terms, 0, unroll=2)

        @pl.loop(0, count)
        def _(v):
            lefts = []
            for i in range(3):
                high, low = halves(force[3 * v + i])
                lefts.append(jnp.concatenate([high, low, high], 1))
            result = dot_nt(jnp.concatenate(lefts, 0), three(back_own[...]))
            for i in range(3):
                for side in range(2):
                    tiles = [
                        result[ROWS * i + q * BX : ROWS * i + (q + 1) * BX, 128 * side : 128 * (side + 1)]
                        for q in range(QY)
                    ]
                    for h, tile in enumerate(swap_strips(tiles)):
                        outs[4 * side + h][3 * v + i] = tile

    vmem = pl.BlockSpec(memory_space=pltpu.VMEM)
    extra = [] if keep else [earlier]
    grid_fields = jax.ShapeDtypeStruct((6 * count, ROWS, NZ), F32)
    scratch = [
        pltpu.VMEM((3 * count, ROWS, NZ), F32),
        pltpu.VMEM((3 * NZ, NZ), BF16),
        pltpu.VMEM((3 * NZ, NZ), BF16),
        pltpu.VMEM((NZ, 2 * NZ), BF16),
    ]
    if not keep:
        scratch.append(pltpu.VMEM((6 * count, ROWS, NZ), F32))
    result = pl.pallas_call(
        kernel,
        name="z_stage_first" if keep else "z_stage_second",
        in_specs=[pl.BlockSpec(memory_space=pltpu.SMEM)] + [vmem] * (len(inputs) + 2 + len(extra)),
        out_shape=[jax.ShapeDtypeStruct((3 * count, BX, 128), F32)] * GZ + ([grid_fields] if keep else []),
        scratch_shapes=scratch,
    )(position, *[near(a) for a in inputs], value, slope, *extra)
    return result[:GZ], (result[GZ] if keep else None)


def x_backward(received, value, position):
    fields = received[0].shape[0]

    def kernel(*refs):
        position_ref = refs[0]
        in_refs = refs[1 : 1 + GZ]
        value_ref, out_ref, lines = refs[1 + GZ :]
        for k in range(GZ):
            start = pl.multiple_of((position_ref[0] ^ k) * BX, BX)
            lines[:, pl.ds(start, BX), :] = in_refs[k][...]
        for pair in range(fields // 2):
            parts = [halves(lines[2 * pair + i]) for i in range(2)]
            high = jnp.concatenate([p[0] for p in parts], 1)
            low = jnp.concatenate([p[1] for p in parts], 1)
            result = dot(three(value_ref[...]), jnp.concatenate([high, low, high], 0))
            for i in range(2):
                out_ref[:, 2 * pair + i] = result[:, 128 * i : 128 * (i + 1)].reshape(GX, LX, 128)

    vmem = pl.BlockSpec(memory_space=pltpu.VMEM)
    return pl.pallas_call(
        kernel,
        name="x_backward",
        in_specs=[pl.BlockSpec(memory_space=pltpu.SMEM)] + [vmem] * (GZ + 1),
        out_shape=jax.ShapeDtypeStruct((GX, fields, LX, 128), F32),
        scratch_shapes=[pltpu.VMEM((fields, NX, 128), F32)],
    )(position, *[near(a) for a in received], value)


PAD = 8
LINES = LX * LZ


def split_inverse(tau_inverse):
    def kernel(in_ref, out_ref):
        @pl.loop(0, LZ, unroll=4)
        def _(m):
            high, low = halves(in_ref[0, m])
            out_ref[0, m] = jnp.concatenate([high, low], 0)

    return pl.pallas_call(
        kernel,
        name="split_inverse",
        grid=(LX,),
        in_specs=[pl.BlockSpec((1, LZ, HALF, NY), lambda i: (i, 0, 0, 0))],
        out_specs=pl.BlockSpec((1, LZ, 2 * HALF, NY), lambda i: (i, 0, 0, 0)),
        out_shape=jax.ShapeDtypeStruct((LX, LZ, 2 * HALF, NY), BF16),
        compiler_params=pltpu.CompilerParams(dimension_semantics=("arbitrary",)),
    )(tau_inverse).reshape(LINES, 2 * HALF, NY)


def finish(received, velocities, gain, keep, inverse, y_back, spread, compact):
    fields = received.shape[1]
    stride = fields * LX
    blocks = 8
    block = LINES // blocks

    def kernel(in_ref, first, second, gain_ref, keep_ref, inverse_far, back_far, spread_far, *refs):
        sources = [first, second]
        outs = refs[:2]
        right, even_part, odd_part, inverse_ref, back_ref, spread_ref, block_sems, back_sem, spread_sem = refs[2:]

        def block_copy(b):
            at = pl.ds(pl.multiple_of(b * block, block), block)
            return pltpu.make_async_copy(inverse_far.at[at], inverse_ref.at[at], block_sems.at[b])

        back_copy = pltpu.make_async_copy(back_far, back_ref, back_sem)
        spread_copy = pltpu.make_async_copy(spread_far, spread_ref, spread_sem)
        back_copy.start()
        for b in range(blocks):
            block_copy(b).start()
        spread_copy.start()

        def lines_of(v, comp):
            f = 3 * v + comp
            quads = []
            for quad in range(2):
                tiles = swap_strips([in_ref[pl.ds(f * LX + quad * 4 + s, GX, stride=stride), :] for s in range(4)])
                quads.append(jnp.concatenate(tiles, 0).T)
            high, low = halves(jnp.concatenate(quads, 0) * gain_ref[...])
            own_high, own_low = halves(sources[v][comp].reshape(LINES, NY))
            return jnp.concatenate([high, low, high, own_high, own_low], 1)

        def put(v, comps, lefts):
            high, low, own = back_ref[0:NY], back_ref[NY : 2 * NY], back_ref[2 * NY : 3 * NY]
            result = dot(jnp.concatenate(lefts, 0), jnp.concatenate([high, high, low, own, own], 0))
            for i, comp in enumerate(comps):
                line = result[LINES * i : LINES * (i + 1)]
                right[pl.ds(3 * v + comp, LINES, stride=PAD), :] = jnp.where(keep_ref[...] > 0.5, line, 0.0)

        for v in range(2):
            if compact:
                if v == 0:
                    back_copy.wait()

                @pl.loop(0, 3)
                def _(comp):
                    put(v, [comp], [lines_of(v, comp)])

            else:
                lefts = [lines_of(v, comp) for comp in range(3)]
                if v == 0:
                    back_copy.wait()
                put(v, range(3), lefts)
        for f in range(fields, PAD):
            right[pl.ds(f, LINES, stride=PAD), :] = jnp.zeros((LINES, NY), F32)

        first_half = lax.broadcasted_iota(jnp.int32, (PAD, NY), 1) < HALF
        zero = jnp.zeros((4 * PAD, NY), BF16)

        @pl.loop(0, blocks)
        def _(b):
            block_copy(b).wait()

            @pl.loop(0, block // 2, unroll=4 if compact else 16)
            def _(step):
                k = b * (block // 2) + step
                lefts = []
                for i in range(2):
                    line = right[pl.ds(pl.multiple_of((2 * k + i) * PAD, PAD), PAD), :]
                    both = jnp.concatenate([jnp.where(first_half, line, 0.0), jnp.where(first_half, 0.0, line)], 0)
                    lefts.append(jnp.concatenate(halves(both), 0))
                left = jnp.concatenate(
                    [jnp.concatenate([lefts[0], zero], 1), jnp.concatenate([zero, lefts[1]], 1)], 0
                )
                weights = jnp.concatenate([inverse_ref[2 * k], inverse_ref[2 * k + 1]], 1)
                result = dot_nt(left, weights)
                for i in range(2):
                    piece = result[4 * PAD * i : 4 * PAD * (i + 1)]
                    piece = piece[: 2 * PAD] + piece[2 * PAD :]
                    at = pl.ds(pl.multiple_of((2 * k + i) * PAD, PAD), PAD)
                    even_part[at, :] = piece[:PAD]
                    odd_part[at, :] = piece[PAD:]

        spread_copy.wait()
        for v in range(2):
            highs, lows = [], []
            for comp in range(3):
                at = pl.ds(3 * v + comp, LINES, stride=PAD)
                high0, low0 = halves(even_part[at, :])
                high1, low1 = halves(odd_part[at, :])
                highs.append(jnp.concatenate([high0, high1], 1))
                lows.append(jnp.concatenate([low0, low1], 1))
            result = dot(jnp.concatenate(highs + lows, 0), spread_ref[...])
            for comp in range(3):
                value = result[LINES * comp : LINES * (comp + 1)] + result[LINES * (3 + comp) : LINES * (4 + comp)]
                outs[v][comp] = value.reshape(LX, LZ, NY)

    vmem = pl.BlockSpec(memory_space=pltpu.VMEM)
    far = pl.BlockSpec(memory_space=pltpu.HBM)
    operands = (received.reshape(GX * stride, 128), *velocities, gain, keep)
    return pl.pallas_call(
        kernel,
        name="finish",
        in_specs=[vmem] * 5 + [far] * 3,
        out_shape=[jax.ShapeDtypeStruct((3, LX, LZ, NY), F32) for _ in range(2)],
        scratch_shapes=[pltpu.VMEM((LINES * PAD, NY), F32) for _ in range(3)]
        + [pltpu.VMEM(a.shape, a.dtype) for a in (inverse, y_back, spread)]
        + [pltpu.SemaphoreType.DMA((blocks,)), pltpu.SemaphoreType.DMA, pltpu.SemaphoreType.DMA],
        compiler_params=pltpu.CompilerParams(vmem_limit_bytes=44 * 1024 * 1024),
    )(*[near(a) for a in operands], *[pltpu.with_memory_space_constraint(a, pltpu.HBM) for a in (inverse, y_back, spread)])


def exchange(array, axis):
    return lax.all_to_all(array, axis, split_axis=0, concat_axis=0, tiled=True)


def exchange_parts(parts):
    return [parts[0]] + [lax.ppermute(parts[k], "pz", [(i, i ^ k) for i in range(GZ)]) for k in range(1, GZ)]


def body(base, adjoint, tangent, second, dealias_mask, tau_rows, tau_inverse):
    table = tables()
    one = [base, adjoint]
    two = [tangent.reshape(adjoint.shape), second.reshape(adjoint.shape)]
    position = lax.axis_index("pz").astype(jnp.int32).reshape(1)
    gain = jnp.broadcast_to((step_gain * dealias_mask.astype(F32)).reshape(LX * LZ, 1), (LX * LZ, NY))
    rows = tau_rows.reshape(LX * LZ, 2)[:, :, None]
    keep = (jnp.arange(HALF, dtype=jnp.int32) != rows).astype(F32).reshape(LX * LZ, NY)
    sent_one = y_forward(one, table["y_first"], False)
    whole_one = exchange(sent_one, "px")
    sent_two = y_forward(two, table["y_first"], True)
    inverse = split_inverse(tau_inverse)
    whole_two = exchange(sent_two, "px")
    parts_one = x_forward(whole_one, table["value"], table["x_slope"], position)
    lines_one = exchange_parts(parts_one)
    partial_two = x_forward(whole_two, table["value"], table["x_slope"])
    lines_two = exchange(partial_two, "pz")
    back_one, grid_one = z_stage(lines_one, table["value"], table["z_slope"], position)
    mixed_one = exchange_parts(back_one)
    modes_one = x_backward(mixed_one, table["value"], position)
    nodes_one = exchange(modes_one, "px")
    back_two, _ = z_stage(
        lines_two, table["value"], table["z_slope"], position, grid_one
    )
    mixed_two = exchange_parts(back_two)
    modes_two = x_backward(mixed_two, table["value"], position)
    nodes_two = exchange(modes_two, "px")
    outs = finish(nodes_one, one, gain, keep, inverse, table["y_back"], table["spread"], True)
    outs += finish(nodes_two, two, gain, keep, inverse, table["y_back"], table["spread"], False)
    return (outs[0], outs[1], outs[2].reshape(tangent.shape), outs[3].reshape(second.shape))


def solution(mesh):
    in_specs = (
        P(None, "px", "pz", None),
        P(None, "px", "pz", None),
        P(None, None, "px", "pz", None),
        P(None, None, "px", "pz", None),
        P("px", "pz"),
        P("px", "pz", None),
        P("px", "pz", None, None),
    )
    out_specs = (
        P(None, "px", "pz", None),
        P(None, "px", "pz", None),
        P(None, None, "px", "pz", None),
        P(None, None, "px", "pz", None),
    )
    return jax.shard_map(body, mesh=mesh, in_specs=in_specs, out_specs=out_specs, check_vma=False)
```

```python
import math

import jax
import jax.numpy as jnp
import numpy as np
from jax import lax
from jax.experimental import pallas as pl
from jax.experimental.pallas import tpu as pltpu
from jax.sharding import PartitionSpec as P

NX = 256
NZ = 256
NY = 128
HALF = 64
GX = 32
GZ = 8
LX = NX // GX
LZ = NZ // GZ
QY = NY // GX
BX = NX // GZ
F32 = jnp.float32
BF16 = jnp.bfloat16

step_gain = 0.5


def split_table(table):
    table = np.asarray(table, np.float32)
    high = table.astype(jnp.bfloat16)
    low = (table - high.astype(np.float32)).astype(jnp.bfloat16)
    return high, low


def hartley(length):
    index = np.arange(length)
    angle = (index[:, None] * index[None, :] % length) * (2.0 * math.pi / length)
    return (np.cos(angle) + np.sin(angle)) / math.sqrt(length)


def hartley_slope(length):
    index = np.arange(length)
    angle = (index[:, None] * index[None, :] % length) * (2.0 * math.pi / length)
    signed = np.where(index < length // 2, index, index - length)
    return (np.cos(angle) - np.sin(angle)) * (signed * (2.0 * math.pi / length))[None, :] / math.sqrt(length)


def chebyshev(length):
    index = np.arange(length)
    angle = ((2 * index[:, None] + 1) * index[None, :] % (4 * length)) * (math.pi / (2 * length))
    scale = np.where(index == 0, math.sqrt(1.0 / length), math.sqrt(2.0 / length))
    return np.cos(angle) * scale[None, :]


def chebyshev_slope(length):
    index = np.arange(length)
    angle = ((2 * index[:, None] + 1) * index[None, :] % (4 * length)) * (math.pi / (2 * length))
    nodes = np.sin((2 * index + 1) * (math.pi / (2 * length)))
    scale = np.where(index == 0, math.sqrt(1.0 / length), math.sqrt(2.0 / length)) * index
    return np.sin(angle) * scale[None, :] / (length * nodes[:, None])


def node_order():
    return (np.arange(GX)[None, :] * QY + np.arange(QY)[:, None]).reshape(-1)


def parity_order():
    return (2 * np.arange(HALF)[None, :] + np.arange(2)[:, None]).reshape(-1)


def beside(table):
    return np.concatenate(split_table(table), 1)


def tables():
    nodes = node_order()
    cheb = chebyshev(NY)
    both = np.concatenate([cheb[nodes], chebyshev_slope(NY)[nodes]], 0)
    order = parity_order()
    gather = (np.arange(NY)[:, None] == order[None, :]).astype(jnp.bfloat16)
    place = gather.T
    even, odd = place[:HALF], place[HALF:]
    return dict(
        y_first=beside(both),
        value=beside(hartley(NX)),
        x_slope=beside(hartley_slope(NX)),
        z_slope=beside(hartley_slope(NZ).T),
        y_back=np.concatenate([*split_table(cheb[nodes][:, order]), gather], 0),
        spread=np.concatenate([even, even, odd, odd], 0),
    )


def three(table):
    half = table.shape[1] // 2
    return jnp.concatenate([table[:, :half], table[:, :half], table[:, half:]], 1)


def near(array):
    return pltpu.with_memory_space_constraint(array, pltpu.VMEM)


def dot(left, right):
    return lax.dot_general(left, right, (((1,), (0,)), ((), ())), preferred_element_type=F32)


def dot_nt(left, right):
    return lax.dot_general(left, right, (((1,), (1,)), ((), ())), preferred_element_type=F32)


def halves(array):
    high = array.astype(BF16)
    return high, (array - high.astype(F32)).astype(BF16)


def swap_strips(tiles):
    lane = lax.broadcasted_iota(jnp.int32, tiles[0].shape, 1)
    low = lane < 64
    even = (lane & 32) == 0
    first, second, third, fourth = tiles
    a = jnp.where(low, first, pltpu.roll(third, 64, 1))
    c = jnp.where(low, pltpu.roll(first, 64, 1), third)
    b = jnp.where(low, second, pltpu.roll(fourth, 64, 1))
    d = jnp.where(low, pltpu.roll(second, 64, 1), fourth)
    return [
        jnp.where(even, a, pltpu.roll(b, 32, 1)),
        jnp.where(even, pltpu.roll(a, 96, 1), b),
        jnp.where(even, c, pltpu.roll(d, 32, 1)),
        jnp.where(even, pltpu.roll(c, 96, 1), d),
    ]


def y_forward(velocities, first, compact):
    count = len(velocities)
    stride = 5 * count * LX

    def kernel(*refs):
        sources, first_ref, out_ref = refs[:count], refs[count], refs[count + 1]

        def one(source, rows, fields):
            high, low = halves(source.reshape(LX * LZ, NY))
            result = dot_nt(three(first_ref[0:rows]), jnp.concatenate([high, low, high], 1))
            for part, field in enumerate(fields):
                for quad in range(2):
                    tiles = [
                        result[part * NY + q * GX : part * NY + (q + 1) * GX, quad * 128 : (quad + 1) * 128]
                        for q in range(QY)
                    ]
                    for s, tile in enumerate(swap_strips(tiles)):
                        out_ref[pl.ds(field * LX + quad * 4 + s, GX, stride=stride), :] = tile

        for v in range(count):

            if compact:

                @pl.loop(0, 2)
                def _(i):
                    one(sources[v][2 * i], 2 * NY, (5 * v + 2 * i, 5 * v + 3 + i))

            else:
                for i in range(2):
                    one(sources[v][2 * i], 2 * NY, (5 * v + 2 * i, 5 * v + 3 + i))

            one(sources[v][1], NY, (5 * v + 1,))

    out = pl.pallas_call(
        kernel,
        name="y_forward",
        out_shape=jax.ShapeDtypeStruct((GX * stride, 128), F32),
    )(*velocities, first)
    return out.reshape(GX, 5 * count, LX, 128)


def fill_blocks(target_ref, first_row, source_ref, first_lane, lanes, position):
    for k in range(GZ):
        start = pl.multiple_of((position ^ k) * BX, BX)
        row = first_row + k * BX
        target_ref[row : row + BX, :] = source_ref[pl.ds(start, BX), first_lane : first_lane + lanes]


def fill_rows(target_ref, source_ref, position):
    for group, lane in enumerate((0, 0, NZ)):
        fill_blocks(target_ref, group * NZ, source_ref, lane, NZ, position)


def x_forward(received, value, slope, position=None):
    count = received.shape[1] // 5
    parts_out = position is not None

    def kernel(*refs):
        if parts_out:
            position_ref, in_ref, value_ref, slope_ref = refs[:4]
            outs = refs[4 : 4 + GZ]
            value_own, slope_own = refs[4 + GZ :]
            fill_blocks(value_own, 0, value_ref, 0, 2 * NX, position_ref[0])
            fill_blocks(slope_own, 0, slope_ref, 0, 2 * NX, position_ref[0])
        else:
            in_ref, value_own, slope_own, out_ref = refs

        @pl.loop(0, count)
        def _(v):
            parts = [halves(in_ref[:, 5 * v + i].reshape(NX, 128)) for i in range(5)]
            high = jnp.concatenate([p[0] for p in parts], 1)
            low = jnp.concatenate([p[1] for p in parts], 1)
            stack = jnp.concatenate([high, low, high], 0)
            plain = dot(three(value_own[...]), stack)
            slopes = dot(three(slope_own[...]), stack[:, 128:384])
            u, vv, w, dyu, dyw = [plain[:, 128 * i : 128 * (i + 1)] for i in range(5)]
            dxv, dxw = slopes[:, :128], slopes[:, 128:]
            for i, piece in enumerate([u, vv, w, dyw, dxw, dxv - dyu]):
                if parts_out:
                    for k in range(GZ):
                        outs[k][6 * v + i] = piece[k * BX : (k + 1) * BX]
                else:
                    out_ref[:, 6 * v + i] = piece.reshape(GZ, BX, 128)

    vmem = pl.BlockSpec(memory_space=pltpu.VMEM)
    if parts_out:
        return pl.pallas_call(
            kernel,
            name="x_forward_parts",
            in_specs=[pl.BlockSpec(memory_space=pltpu.SMEM), vmem, vmem, vmem],
            out_shape=[jax.ShapeDtypeStruct((6 * count, BX, 128), F32)] * GZ,
            scratch_shapes=[pltpu.VMEM((NX, 2 * NX), BF16), pltpu.VMEM((NX, 2 * NX), BF16)],
        )(position, near(received), value, slope)
    return pl.pallas_call(
        kernel,
        name="x_forward",
        in_specs=[vmem, vmem, vmem],
        out_shape=jax.ShapeDtypeStruct((GZ, 6 * count, BX, 128), F32),
    )(near(received), near(value), near(slope))


ROWS = QY * BX


def cross(velocity, vortex):
    return [
        velocity[(i + 1) % 3] * vortex[(i + 2) % 3] - velocity[(i + 2) % 3] * vortex[(i + 1) % 3] for i in range(3)
    ]


def added(*terms):
    result = terms[0]
    for term in terms[1:]:
        result = [a + b for a, b in zip(result, term)]
    return result


def z_stage(received, value, slope, position, earlier=None):
    split_in = isinstance(received, (list, tuple))
    inputs = list(received) if split_in else [received]
    count = 2
    keep = earlier is None

    def kernel(*refs):
        position_ref = refs[0]
        in_refs = refs[1 : 1 + len(inputs)]
        at = 1 + len(inputs)
        value_ref, slope_ref = refs[at : at + 2]
        at += 2
        if not keep:
            old = refs[at]
            at += 1
        outs = refs[at : at + GZ]
        at += GZ
        if keep:
            phys = refs[at]
            at += 1
        force, value_own, slope_own, back_own = refs[at : at + 4]
        if not keep:
            phys = refs[at + 4]
        fill_blocks(back_own, 0, value_ref, 0, 2 * NZ, position_ref[0])
        order = position_ref[0] if split_in else 0
        fill_rows(value_own, value_ref, order)
        fill_rows(slope_own, slope_ref, order)
        if split_in:
            source = lambda block, field: in_refs[block][field]
        else:
            source = lambda block, field: in_refs[0][block, field]

        @pl.loop(0, count)
        def _(v):
            lefts = []
            for i in range(6):
                sides = [swap_strips([source(4 * side + h, 6 * v + i) for h in range(4)]) for side in range(2)]
                lines = jnp.concatenate(
                    [jnp.concatenate([sides[0][q], sides[1][q]], 1) for q in range(QY)], 0
                )
                high, low = halves(lines)
                lefts.append(jnp.concatenate([high, low, high], 1))
            values = dot(jnp.concatenate(lefts, 0), value_own[...])
            slopes = dot(jnp.concatenate(lefts[0:2], 0), slope_own[...])
            pieces = [values[ROWS * i : ROWS * (i + 1)] for i in range(6)]
            pieces[3] = pieces[3] - slopes[ROWS:]
            pieces[4] = slopes[:ROWS] - pieces[4]
            for i in range(6):
                phys[6 * v + i] = pieces[i]

        def cross_terms(r, carry):
            rows = pl.ds(pl.multiple_of(r * 8, 8), 8)
            new = [phys[i, rows, :] for i in range(12)]
            if keep:
                base_v, base_o, adj_v, adj_o = new[0:3], new[3:6], new[6:9], new[9:12]
                results = cross(base_v, base_o) + added(cross(base_v, adj_o), cross(adj_v, base_o))
            else:
                past = [old[i, rows, :] for i in range(12)]
                base_v, base_o, adj_v, adj_o = past[0:3], past[3:6], past[6:9], past[9:12]
                tang_v, tang_o, sec_v, sec_o = new[0:3], new[3:6], new[6:9], new[9:12]
                results = added(cross(base_v, tang_o), cross(tang_v, base_o)) + added(
                    cross(base_v, sec_o), cross(sec_v, base_o), cross(tang_v, adj_o), cross(adj_v, tang_o)
                )
            for i, piece in enumerate(results):
                force[i, rows, :] = piece
            return carry

        lax.fori_loop(0, ROWS // 8, cross_terms, 0, unroll=2)

        @pl.loop(0, count)
        def _(v):
            lefts = []
            for i in range(3):
                high, low = halves(force[3 * v + i])
                lefts.append(jnp.concatenate([high, low, high], 1))
            result = dot_nt(jnp.concatenate(lefts, 0), three(back_own[...]))
            for i in range(3):
                for side in range(2):
                    tiles = [
                        result[ROWS * i + q * BX : ROWS * i + (q + 1) * BX, 128 * side : 128 * (side + 1)]
                        for q in range(QY)
                    ]
                    for h, tile in enumerate(swap_strips(tiles)):
                        outs[4 * side + h][3 * v + i] = tile

    vmem = pl.BlockSpec(memory_space=pltpu.VMEM)
    extra = [] if keep else [earlier]
    grid_fields = jax.ShapeDtypeStruct((6 * count, ROWS, NZ), F32)
    scratch = [
        pltpu.VMEM((3 * count, ROWS, NZ), F32),
        pltpu.VMEM((3 * NZ, NZ), BF16),
        pltpu.VMEM((3 * NZ, NZ), BF16),
        pltpu.VMEM((NZ, 2 * NZ), BF16),
    ]
    if not keep:
        scratch.append(pltpu.VMEM((6 * count, ROWS, NZ), F32))
    result = pl.pallas_call(
        kernel,
        name="z_stage_first" if keep else "z_stage_second",
        in_specs=[pl.BlockSpec(memory_space=pltpu.SMEM)] + [vmem] * (len(inputs) + 2 + len(extra)),
        out_shape=[jax.ShapeDtypeStruct((3 * count, BX, 128), F32)] * GZ + ([grid_fields] if keep else []),
        scratch_shapes=scratch,
    )(position, *[near(a) for a in (*inputs, value, slope)], *extra)
    return result[:GZ], (result[GZ] if keep else None)


def x_backward(received, value, position):
    fields = received[0].shape[0]

    def kernel(*refs):
        position_ref = refs[0]
        in_refs = refs[1 : 1 + GZ]
        value_ref, out_ref, lines = refs[1 + GZ :]
        for k in range(GZ):
            start = pl.multiple_of((position_ref[0] ^ k) * BX, BX)
            lines[:, pl.ds(start, BX), :] = in_refs[k][...]
        for pair in range(fields // 2):
            parts = [halves(lines[2 * pair + i]) for i in range(2)]
            high = jnp.concatenate([p[0] for p in parts], 1)
            low = jnp.concatenate([p[1] for p in parts], 1)
            result = dot(three(value_ref[...]), jnp.concatenate([high, low, high], 0))
            for i in range(2):
                out_ref[:, 2 * pair + i] = result[:, 128 * i : 128 * (i + 1)].reshape(GX, LX, 128)

    vmem = pl.BlockSpec(memory_space=pltpu.VMEM)
    return pl.pallas_call(
        kernel,
        name="x_backward",
        in_specs=[pl.BlockSpec(memory_space=pltpu.SMEM)] + [vmem] * (GZ + 1),
        out_shape=jax.ShapeDtypeStruct((GX, fields, LX, 128), F32),
        scratch_shapes=[pltpu.VMEM((fields, NX, 128), F32)],
    )(position, *[near(a) for a in received], near(value))


PAD = 8
LINES = LX * LZ


def split_inverse(tau_inverse):
    def kernel(in_ref, out_ref):
        @pl.loop(0, LZ, unroll=4)
        def _(m):
            high, low = halves(in_ref[0, m])
            out_ref[0, m] = jnp.concatenate([high, low], 0)

    return pl.pallas_call(
        kernel,
        name="split_inverse",
        grid=(LX,),
        in_specs=[pl.BlockSpec((1, LZ, HALF, NY), lambda i: (i, 0, 0, 0))],
        out_specs=pl.BlockSpec((1, LZ, 2 * HALF, NY), lambda i: (i, 0, 0, 0)),
        out_shape=jax.ShapeDtypeStruct((LX, LZ, 2 * HALF, NY), BF16),
        compiler_params=pltpu.CompilerParams(dimension_semantics=("arbitrary",)),
    )(tau_inverse).reshape(LINES, 2 * HALF, NY)


def finish(received, velocities, gain, keep, inverse, y_back, spread, compact):
    fields = received.shape[1]
    stride = fields * LX
    blocks = 8
    block = LINES // blocks

    def kernel(in_ref, first, second, gain_ref, keep_ref, inverse_far, back_far, spread_far, *refs):
        sources = [first, second]
        outs = refs[:2]
        right, even_part, odd_part, inverse_ref, back_ref, spread_ref, block_sems, back_sem, spread_sem = refs[2:]

        def block_copy(b):
            at = pl.ds(pl.multiple_of(b * block, block), block)
            return pltpu.make_async_copy(inverse_far.at[at], inverse_ref.at[at], block_sems.at[b])

        back_copy = pltpu.make_async_copy(back_far, back_ref, back_sem)
        spread_copy = pltpu.make_async_copy(spread_far, spread_ref, spread_sem)
        back_copy.start()
        for b in range(blocks):
            block_copy(b).start()
        spread_copy.start()

        def lines_of(v, comp):
            f = 3 * v + comp
            quads = []
            for quad in range(2):
                tiles = swap_strips([in_ref[pl.ds(f * LX + quad * 4 + s, GX, stride=stride), :] for s in range(4)])
                quads.append(jnp.concatenate(tiles, 0).T)
            high, low = halves(jnp.concatenate(quads, 0) * gain_ref[...])
            own_high, own_low = halves(sources[v][comp].reshape(LINES, NY))
            return jnp.concatenate([high, low, high, own_high, own_low], 1)

        def put(v, comps, lefts):
            high, low, own = back_ref[0:NY], back_ref[NY : 2 * NY], back_ref[2 * NY : 3 * NY]
            result = dot(jnp.concatenate(lefts, 0), jnp.concatenate([high, high, low, own, own], 0))
            for i, comp in enumerate(comps):
                line = result[LINES * i : LINES * (i + 1)]
                right[pl.ds(3 * v + comp, LINES, stride=PAD), :] = jnp.where(keep_ref[...] > 0.5, line, 0.0)

        for v in range(2):
            if compact:
                if v == 0:
                    back_copy.wait()

                @pl.loop(0, 3)
                def _(comp):
                    put(v, [comp], [lines_of(v, comp)])

            else:
                lefts = [lines_of(v, comp) for comp in range(3)]
                if v == 0:
                    back_copy.wait()
                put(v, range(3), lefts)
        for f in range(fields, PAD):
            right[pl.ds(f, LINES, stride=PAD), :] = jnp.zeros((LINES, NY), F32)

        first_half = lax.broadcasted_iota(jnp.int32, (PAD, NY), 1) < HALF
        zero = jnp.zeros((4 * PAD, NY), BF16)

        @pl.loop(0, blocks)
        def _(b):
            block_copy(b).wait()

            @pl.loop(0, block // 2, unroll=4 if compact else 16)
            def _(step):
                k = b * (block // 2) + step
                lefts = []
                for i in range(2):
                    line = right[pl.ds(pl.multiple_of((2 * k + i) * PAD, PAD), PAD), :]
                    both = jnp.concatenate([jnp.where(first_half, line, 0.0), jnp.where(first_half, 0.0, line)], 0)
                    lefts.append(jnp.concatenate(halves(both), 0))
                left = jnp.concatenate(
                    [jnp.concatenate([lefts[0], zero], 1), jnp.concatenate([zero, lefts[1]], 1)], 0
                )
                weights = jnp.concatenate([inverse_ref[2 * k], inverse_ref[2 * k + 1]], 1)
                result = dot_nt(left, weights)
                for i in range(2):
                    piece = result[4 * PAD * i : 4 * PAD * (i + 1)]
                    piece = piece[: 2 * PAD] + piece[2 * PAD :]
                    at = pl.ds(pl.multiple_of((2 * k + i) * PAD, PAD), PAD)
                    even_part[at, :] = piece[:PAD]
                    odd_part[at, :] = piece[PAD:]

        spread_copy.wait()
        for v in range(2):
            highs, lows = [], []
            for comp in range(3):
                at = pl.ds(3 * v + comp, LINES, stride=PAD)
                high0, low0 = halves(even_part[at, :])
                high1, low1 = halves(odd_part[at, :])
                highs.append(jnp.concatenate([high0, high1], 1))
                lows.append(jnp.concatenate([low0, low1], 1))
            result = dot(jnp.concatenate(highs + lows, 0), spread_ref[...])
            for comp in range(3):
                value = result[LINES * comp : LINES * (comp + 1)] + result[LINES * (3 + comp) : LINES * (4 + comp)]
                outs[v][comp] = value.reshape(LX, LZ, NY)

    vmem = pl.BlockSpec(memory_space=pltpu.VMEM)
    far = pl.BlockSpec(memory_space=pltpu.HBM)
    operands = (received.reshape(GX * stride, 128), *velocities, gain, keep)
    return pl.pallas_call(
        kernel,
        name="finish",
        in_specs=[vmem] * 5 + [far] * 3,
        out_shape=[jax.ShapeDtypeStruct((3, LX, LZ, NY), F32) for _ in range(2)],
        scratch_shapes=[pltpu.VMEM((LINES * PAD, NY), F32) for _ in range(3)]
        + [pltpu.VMEM(a.shape, a.dtype) for a in (inverse, y_back, spread)]
        + [pltpu.SemaphoreType.DMA((blocks,)), pltpu.SemaphoreType.DMA, pltpu.SemaphoreType.DMA],
        compiler_params=pltpu.CompilerParams(vmem_limit_bytes=44 * 1024 * 1024),
    )(*[near(a) for a in operands], *[pltpu.with_memory_space_constraint(a, pltpu.HBM) for a in (inverse, y_back, spread)])


def exchange(array, axis):
    return lax.all_to_all(array, axis, split_axis=0, concat_axis=0, tiled=True)


def exchange_parts(parts):
    return [parts[0]] + [lax.ppermute(parts[k], "pz", [(i, i ^ k) for i in range(GZ)]) for k in range(1, GZ)]


def body(base, adjoint, tangent, second, dealias_mask, tau_rows, tau_inverse):
    table = tables()
    one = [base, adjoint]
    two = [tangent.reshape(adjoint.shape), second.reshape(adjoint.shape)]
    position = lax.axis_index("pz").astype(jnp.int32).reshape(1)
    gain = jnp.broadcast_to((step_gain * dealias_mask.astype(F32)).reshape(LX * LZ, 1), (LX * LZ, NY))
    rows = tau_rows.reshape(LX * LZ, 2)[:, :, None]
    keep = (jnp.arange(HALF, dtype=jnp.int32) != rows).astype(F32).reshape(LX * LZ, NY)
    sent_one = y_forward(one, table["y_first"], False)
    whole_one = exchange(sent_one, "px")
    sent_two = y_forward(two, table["y_first"], True)
    inverse = split_inverse(tau_inverse)
    whole_two = exchange(sent_two, "px")
    parts_one = x_forward(whole_one, table["value"], table["x_slope"], position)
    lines_one = exchange_parts(parts_one)
    partial_two = x_forward(whole_two, table["value"], table["x_slope"])
    lines_two = exchange(partial_two, "pz")
    back_one, grid_one = z_stage(lines_one, table["value"], table["z_slope"], position)
    mixed_one = exchange_parts(back_one)
    modes_one = x_backward(mixed_one, table["value"], position)
    nodes_one = exchange(modes_one, "px")
    back_two, _ = z_stage(
        lines_two, table["value"], table["z_slope"], position, grid_one
    )
    mixed_two = exchange_parts(back_two)
    modes_two = x_backward(mixed_two, table["value"], position)
    nodes_two = exchange(modes_two, "px")
    outs = finish(nodes_one, one, gain, keep, inverse, table["y_back"], table["spread"], True)
    outs += finish(nodes_two, two, gain, keep, inverse, table["y_back"], table["spread"], False)
    return (outs[0], outs[1], outs[2].reshape(tangent.shape), outs[3].reshape(second.shape))


def solution(mesh):
    in_specs = (
        P(None, "px", "pz", None),
        P(None, "px", "pz", None),
        P(None, None, "px", "pz", None),
        P(None, None, "px", "pz", None),
        P("px", "pz"),
        P("px", "pz", None),
        P("px", "pz", None, None),
    )
    out_specs = (
        P(None, "px", "pz", None),
        P(None, "px", "pz", None),
        P(None, None, "px", "pz", None),
        P(None, None, "px", "pz", None),
    )
    return jax.shard_map(body, mesh=mesh, in_specs=in_specs, out_specs=out_specs, check_vma=False)
```
